32 devices in a mesh: dp: 8 (over z, x), tensor: 4 (over y, core).
Axes of the slice: x: 2, y: 2, z: 4, core: 2. Of those that a mesh axis runs over, the one named last changes fastest.
Arguments:
- tokens: bfloat16 [2, 512, 4096], P(None, 'dp', 'tensor'), may hold values from -6 to 6
- routes: int32 [2, 512, 2], P(None, 'dp'), may hold values from 0 to 7, all different within a row; in each aligned block of 64 rows (0 to 63, 64 to 127, ..., all dimensions but the last counted through in order) at most 20 rows name the same one
- probs: float32 [2, 512, 8], P(None, 'dp'), may hold values from 0 to 1, as said below
- w_gate: bfloat16 [8, 4096, 14336], P('dp', None, 'tensor'), may hold values from -0.09375 to 0.09375
- w_up: bfloat16 [8, 4096, 14336], P('dp', None, 'tensor'), may hold values from -0.09375 to 0.09375
- w_down: bfloat16 [8, 14336, 4096], P('dp', 'tensor'), may hold values from -0.046875 to 0.046875
Outputs:
- mixed: bfloat16 [2, 512, 4096], P(None, 'dp', 'tensor')
- aux_loss: float32 [2, 8], replicated
The draws below stay inside these ranges and needn't reach their ends.
Inputs may be any that keep to these rules, and one draw needn't show every extreme that they name: `routes`: in each aligned block of 64 rows (the rows of one index of dp in one micro-batch) no expert is named in more than 20 entries; the 2 experts of a row differ. `probs`: each row is positive and sums to one.
All inputs are finite; a program needn't handle non-finite values.
Results may differ from the reference program's by a relative error of at most 0.012.
Values may be sent and summed in bfloat16 or wider, within the bound.
No kernel may reach another device: no remote copies, remote signals or barrier semaphores. Data moves between devices by JAX's collectives and lax.ppermute only.
A program may use at most 192 MiB of HBM per device.

```python
import math
import jax
import jax.numpy as jnp
import numpy as np
from jax import lax

D = 4096
FF = 14336
EXPERTS = 8
TOP = 2
MICRO = 2
MB_DEV = 64
CAP = 20
MB_TOK = 512
BLOCKS = 8
FF_BLK = 14336
N_DP = 8
N_TENSOR = 4


def draw_probs(key, part):
    first, second, third = jax.random.split(jax.random.fold_in(key, 71), 3)
    group_count = MB_TOK // MB_DEV
    group = jnp.arange(MB_TOK, dtype=jnp.int32) // MB_DEV
    along = group.astype(jnp.float32) / max(group_count - 1, 1)
    micro_ids = jnp.arange(MICRO, dtype=jnp.int32)
    expert_ids = jnp.arange(EXPERTS, dtype=jnp.int32)
    leading = (micro_ids * 3 + 1) % EXPERTS
    marked = (leading[:, None, None] == expert_ids[None, None, :]).astype(jnp.float32)
    rotating = (group[None, :] + micro_ids[:, None] * 5 + 2) % EXPERTS
    second_mark = (rotating[:, :, None] == expert_ids[None, None, :]).astype(jnp.float32)
    common = 0.5 * jax.random.normal(third, (1, 1, EXPERTS), jnp.float32)
    noise = jax.random.normal(first, (MICRO, MB_TOK, EXPERTS), jnp.float32)
    strength = 1.0 + 4.0 * along
    row_scale = jnp.exp(jax.random.uniform(second, (MICRO, MB_TOK, 1), jnp.float32, 0.0, jnp.log(2.0)))
    logits = noise * row_scale * 0.5 + strength[None, :, None] * marked + second_mark + common
    return jax.nn.softmax(logits, axis=-1).astype(jnp.float32)


def shard_levels(own_key, extent, shards, least, high):
    def one(axis_at, blocks):
        steps = jax.random.uniform(jax.random.fold_in(jax.random.fold_in(own_key, 6), axis_at), (blocks,), jnp.float32, least / len(shards), high / len(shards))
        return jnp.repeat(jnp.exp(steps), extent[axis_at] // blocks).reshape((-1,) + (1,) * (len(extent) - axis_at - 1))

    factor_of = one(*shards[0])
    for cut in shards[1:]:
        factor_of = factor_of * one(*cut)
    return factor_of


def deal_out(own_key, own, number, rows, amount, top, limit, slope):
    sequence = jax.random.permutation(own_key, amount)
    crowded, ordinary = load_shares(amount, rows * top, limit, slope, True), load_shares(amount, rows * top, limit, slope, False)
    places = jnp.arange(amount)

    def named(sizes, rotation):
        used = int((sizes > 0).sum())
        fixed = max(1, used // 4)
        moved = fixed + (places - fixed + rotation * (used - fixed)) % max(1, amount - fixed)
        return jnp.zeros((amount,), jnp.int32).at[sequence[jnp.where(places < fixed, places, moved)]].set(jnp.asarray(sizes, jnp.int32))

    sizes = jnp.where(number % 4 == 0, named(crowded, number // 4), named(ordinary, number - number // 4 - 1))
    mixed = jax.random.permutation(jax.random.fold_in(own, 3), amount)
    giver, receiver = mixed[0:amount // 2 * 2:2], mixed[1:amount // 2 * 2:2]
    room = jnp.minimum(sizes[giver] - 1, limit - sizes[receiver]) // 2
    room = jnp.where((giver == sequence[0]) | (receiver == sequence[0]) | (sizes[receiver] == 0), 0, jnp.maximum(room, 0))
    moved = jax.random.randint(jax.random.fold_in(own, 4), (amount // 2,), 0, 1 << 20) % (room + 1)
    sizes = sizes.at[giver].add(-moved).at[receiver].add(moved)
    items = jnp.searchsorted(jnp.cumsum(sizes), jnp.arange(rows * top), side="right").astype(jnp.int32)
    listing = items.reshape(top, rows).T
    listing = listing[jax.random.permutation(jax.random.fold_in(own, 1), rows)]
    rotation = jax.random.randint(jax.random.fold_in(own, 2), (rows, 1), 0, top)
    return jnp.take_along_axis(listing, (jnp.arange(top)[None, :] + rotation) % top, axis=1)


def load_shares(amount, total, reach, lean, full):
    portions = [(1 << 20) // math.isqrt(rank ** lean) + 1 for rank in range(1, amount + 1)]
    largest = reach if full else min(reach, max(-(-total // amount), total * portions[0] // sum(portions)))
    least = 1 if total - largest >= amount - 1 else 0
    given, rest = [largest] + [least] * (amount - 1), total - largest - least * (amount - 1)
    while rest > 0:
        candidates = [i for i in range(1, amount) if given[i] < largest] or [i for i in range(1, amount) if given[i] < reach]
        whole, remaining = sum([portions[i] for i in candidates]), rest
        for i in candidates:
            addition = min(reach - given[i], max(1, remaining * portions[i] // whole), rest)
            given[i] = given[i] + addition
            rest = rest - addition
    return np.array(given)


def bell_draw(own_key, shape, deviation, reach, cuts=(), kind=jnp.bfloat16):
    loudness = shard_levels(own_key, shape, cuts, -0.22, 0.18) if cuts else 1.0
    values = jax.random.normal(own_key, shape, jnp.float32) * deviation * loudness
    return jnp.minimum(jnp.maximum(values, -reach), reach).astype(kind)


def setup_inputs(seed: int = 0) -> dict:
    key_list = jax.random.split(jax.random.key(seed), 7)
    tokens = bell_draw(key_list[0], (MICRO, MB_TOK, D), 1.0, 6.0, ((1, 8), (2, 4)))
    routes_keys = jax.random.split(jax.random.fold_in(key_list[1], 1), MICRO * MB_TOK // MB_DEV)
    routes_turns = jax.random.permutation(jax.random.fold_in(key_list[1], 3), MICRO * MB_TOK // MB_DEV)
    routes = jax.vmap(lambda own, number: deal_out(jax.random.fold_in(key_list[1], 2), own, number, MB_DEV, EXPERTS, TOP, CAP, 1))(routes_keys, routes_turns).reshape((MICRO, MB_TOK, TOP))
    probs = draw_probs(jax.random.fold_in(key_list[6], 71), 0)
    w_gate = bell_draw(key_list[3], (BLOCKS, D, FF_BLK), D ** -0.5, 0.09375, ((0, 8), (2, 4)))
    w_up = bell_draw(key_list[4], (BLOCKS, D, FF_BLK), D ** -0.5, 0.09375, ((0, 8), (2, 4)))
    w_down = bell_draw(key_list[5], (BLOCKS, FF_BLK, D), FF ** -0.5, 0.046875, ((0, 8), (1, 4)))
    return {"tokens": tokens, "routes": routes, "probs": probs, "w_gate": w_gate, "w_up": w_up, "w_down": w_down}


def slot_tables(route, prob):
    rows_count = route.shape[0]
    experts = prob.shape[-1]
    capacity = CAP
    flat = route.reshape(-1)
    onehot = (flat[:, None] == jnp.arange(experts, dtype=jnp.int32)[None, :]).astype(jnp.int32)
    before = jnp.cumsum(onehot, axis=0) - onehot
    place = jnp.sum(before * onehot, axis=1)
    slot = flat * capacity + place
    picked = jnp.take_along_axis(prob, route, axis=1)
    weights = picked / jnp.sum(picked, axis=1, keepdims=True)
    grid = (slot[:, None] == jnp.arange(experts * capacity, dtype=jnp.int32)[None, :]).astype(jnp.float32)
    grid = grid.reshape(rows_count, route.shape[1], experts * capacity)
    dispatch = jnp.sum(grid, axis=1).T.astype(jnp.bfloat16)
    combine = jnp.sum(grid * weights[:, :, None], axis=1)
    counts = jnp.sum(onehot, axis=0).astype(jnp.float32)
    return dispatch, combine, counts


def reference(tokens, routes, probs, w_gate, w_up, w_down):
    per_expert = N_DP // EXPERTS
    quarter = FF // (per_expert * N_TENSOR)
    loss_terms = []
    outputs = []
    for micro_index in range(MICRO):
        tok_groups = tokens[micro_index].reshape(N_DP, MB_DEV, D)
        route_groups = routes[micro_index].reshape(N_DP, MB_DEV, TOP)
        prob_groups = probs[micro_index].reshape(N_DP, MB_DEV, EXPERTS)
        dispatch, combine, counts = jax.vmap(slot_tables)(route_groups, prob_groups)
        slots = jnp.einsum("psr,prd->psd", dispatch.astype(jnp.float32), tok_groups.astype(jnp.float32)).astype(jnp.bfloat16)
        expert_rows = slots.reshape(N_DP, EXPERTS, CAP, D).transpose(1, 0, 2, 3).reshape(EXPERTS, N_DP * CAP, D)

        def one_expert(args):
            expert_id, rows_in = args

            def add_block(block, total):
                sub = (block // N_TENSOR).astype(jnp.int32)
                column = ((block % N_TENSOR) * quarter).astype(jnp.int32)
                index = (expert_id * per_expert + sub).astype(jnp.int32)
                zero = jnp.int32(0)
                gate_block = lax.dynamic_slice(w_gate, (index, zero, column), (1, D, quarter))[0]
                up_block = lax.dynamic_slice(w_up, (index, zero, column), (1, D, quarter))[0]
                down_block = lax.dynamic_slice(w_down, (index, column, zero), (1, quarter, D))[0]
                gate = jnp.dot(rows_in, gate_block, preferred_element_type=jnp.float32)
                up = jnp.dot(rows_in, up_block, preferred_element_type=jnp.float32)
                hidden = (jax.nn.silu(gate) * up).astype(jnp.bfloat16)
                part = jnp.dot(hidden, down_block, preferred_element_type=jnp.float32).astype(jnp.bfloat16)
                part = lax.optimization_barrier(part)
                return total + part.astype(jnp.float32)

            start = jnp.zeros((N_DP * CAP, D), jnp.float32)
            return lax.fori_loop(0, per_expert * N_TENSOR, add_block, start)

        sums = lax.map(one_expert, (jnp.arange(EXPERTS, dtype=jnp.int32), expert_rows))
        sums = sums.reshape(EXPERTS, N_DP, CAP, D).transpose(1, 0, 2, 3).reshape(N_DP, EXPERTS * CAP, D)
        mixed = jnp.einsum("prs,psd->prd", combine, sums, precision=lax.Precision.HIGHEST)
        outputs.append(mixed.reshape(MB_TOK, D).astype(jnp.bfloat16))
        count_all = jnp.sum(counts, axis=0)
        prob_all = jnp.sum(probs[micro_index], axis=0)
        loss_terms.append(EXPERTS * (count_all / (MB_TOK * TOP)) * (prob_all / MB_TOK))
    return jnp.stack(outputs), jnp.stack(loss_terms)
```

```python
import functools

import jax
import jax.numpy as jnp
from jax import lax
from jax.experimental import pallas as pl
from jax.experimental.pallas import tpu as pltpu
from jax.sharding import PartitionSpec as P


CAP = 20
LANES = 128
PAIR_KEY = 64
IN_CHUNKS = 2
OUT_CHUNKS = 2
DOWN_PARTS = 7


def tile_of(size, most):
    return max(d for d in range(LANES, most + 1, LANES) if size % d == 0)


def places(dims, routes_ref, m):
    dp, cap2, experts = dims
    rows = routes_ref.shape[2]
    at = lax.broadcasted_iota(jnp.int32, (dp * cap2, rows), 0).astype(jnp.float32)
    device = jnp.floor((at + 0.5) * (1.0 / cap2))
    keys = jnp.floor((device + 0.5) * (experts / dp)) * PAIR_KEY + (at - device * cap2)
    earlier = lax.broadcasted_iota(jnp.int32, (rows, rows), 0) < lax.broadcasted_iota(
        jnp.int32, (rows, rows), 1
    )
    ids = lax.broadcasted_iota(jnp.int32, (experts, rows), 0)
    route = routes_ref[m]
    hits = [(route[k : k + 1, :] == ids).astype(jnp.float32) for k in range(2)]
    named = hits[0] + hits[1]
    before = jnp.dot(named, earlier.astype(jnp.float32), preferred_element_type=jnp.float32)
    here = []
    for k in range(2):
        place = jnp.sum(before * hits[k], axis=0, keepdims=True)
        own_key = route[k : k + 1, :].astype(jnp.float32) * PAIR_KEY + (m * CAP + place)
        here.append((keys == own_key).astype(jnp.float32))
    return hits, named, here


def tables_kernel(dims, routes_ref, probs_ref, tokens_ref, sent_ref, aux_ref):
    dp, cap2, experts = dims
    micro = routes_ref.shape[0]
    blocks = tokens_ref.shape[2] // LANES
    aux_ref[...] = jnp.zeros_like(aux_ref)
    slots = jnp.zeros((dp * cap2, tokens_ref.shape[2]), jnp.float32)
    for m in range(micro):
        _, named, here = places(dims, routes_ref, m)
        pick = (here[0] + here[1]).astype(jnp.bfloat16)
        slots = slots + jnp.dot(pick, tokens_ref[m], preferred_element_type=jnp.float32)
        sums = jnp.sum(probs_ref[m], axis=1, keepdims=True)
        aux_ref[0:experts, m : m + 1] = jnp.sum(named, axis=1, keepdims=True)
        for piece in range(3):
            part = sums.astype(jnp.bfloat16).astype(jnp.float32)
            column = (piece + 1) * micro + m
            aux_ref[0:experts, column : column + 1] = part
            sums = sums - part
    slots = slots.astype(jnp.bfloat16)
    aux = aux_ref[...].astype(jnp.bfloat16)
    for d in range(dp):
        for b in range(blocks):
            sent_ref[d, b * cap2 : (b + 1) * cap2, :] = slots[
                d * cap2 : (d + 1) * cap2, b * LANES : (b + 1) * LANES
            ]
        sent_ref[d, blocks * cap2 :, :] = aux


def weights_kernel(dims, routes_ref, probs_ref, combine_ref):
    for m in range(routes_ref.shape[0]):
        hits, _, here = places(dims, routes_ref, m)
        picked = [jnp.sum(probs_ref[m] * hit, axis=0, keepdims=True) for hit in hits]
        total = picked[0] + picked[1]
        combine_ref[m] = here[0] * (picked[0] / total) + here[1] * (picked[1] / total)


def repack_kernel(dims, arrived_ref, *refs):
    dp, cap2, blocks, micro, experts, tokens_all = dims
    xs, loss_ref = refs[:-1], refs[-1]
    per = blocks // len(xs)
    total = jnp.zeros((experts, LANES), jnp.float32)
    for d in range(dp):
        for b in range(blocks):
            xs[b // per][
                d * cap2 : (d + 1) * cap2, b % per * LANES : (b % per + 1) * LANES
            ] = arrived_ref[d, b * cap2 : (b + 1) * cap2, :]
        total = total + arrived_ref[d, blocks * cap2 :, :].astype(jnp.float32)
    count = total[:, 0:micro]
    prob = total[:, 3 * micro : 4 * micro] + total[:, 2 * micro : 3 * micro]
    prob = prob + total[:, micro : 2 * micro]
    loss_ref[...] = experts * (count / (tokens_all * 2)) * (prob / tokens_all)


def gate_up_copies(pieces, here, sources, targets, sems):
    copies = []
    depth = targets[0].shape[0] // len(pieces)
    half = depth // 2
    for i, (quarter, c) in enumerate(pieces):
        start = ((here ^ quarter) * IN_CHUNKS + c) * depth
        for k, (source, target) in enumerate(zip(sources, targets)):
            for part in range(2):
                at = pl.multiple_of(start + part * half, half)
                copies.append(
                    pltpu.make_async_copy(
                        source.at[0, pl.ds(at, half), :],
                        target.at[pl.ds(i * depth + part * half, half), :],
                        sems.at[k, 2 * i + part],
                    )
                )
    return copies


def down_copies(side, parts, here, source, targets, sems):
    copies = []
    half, columns = targets[0].shape
    at = pl.multiple_of(((here >> 1) ^ side) * columns, columns)
    step = half // DOWN_PARTS
    for i, target in zip(parts, targets):
        for part in range(DOWN_PARTS):
            copies.append(
                pltpu.make_async_copy(
                    source.at[0, pl.ds(i * half + part * step, step), pl.ds(at, columns)],
                    target.at[pl.ds(part * step, step), :],
                    sems.at[i, part],
                )
            )
    return copies


def run_copies(copies):
    for copy in copies:
        copy.start()

    def finish():
        for copy in copies:
            copy.wait()

    return finish


def first_kernel(pieces, where_ref, after_ref, w_gate, w_up, gate_ref, up_ref, sems):
    sources, targets = (w_gate, w_up), (gate_ref, up_ref)
    run_copies(gate_up_copies(pieces, where_ref[0], sources, targets, sems))()


def gate_up_kernel(plan, where_ref, *refs):
    count, first, following, tile = plan
    last = following is None
    xs, refs = refs[:count], refs[count:]
    gate_w, up_w, refs = refs[0], refs[1], refs[2:]
    if not first:
        gate_in, up_in, refs = refs[0], refs[1], refs[2:]
    here = where_ref[0]
    if last:
        w_down, out_ref, next_a, next_b, sems = refs
        copies = down_copies(1, (0, 1), here, w_down, (next_a, next_b), sems)
    else:
        w_gate, w_up, gate_out, up_out, next_a, next_b, sems = refs
        copies = gate_up_copies(following, here, (w_gate, w_up), (next_a, next_b), sems)
    finish = run_copies(copies)
    depth = gate_w.shape[0] // count

    def step(j, carry):
        columns = pl.ds(pl.multiple_of(j * tile, tile), tile)
        if first:
            gate = up = 0.0
        else:
            gate, up = gate_in[:, columns], up_in[:, columns]
        for i, x in enumerate(xs):
            rows = slice(i * depth, (i + 1) * depth)
            gate = gate + jnp.dot(
                x[...], gate_w[rows, columns], preferred_element_type=jnp.float32
            )
            up = up + jnp.dot(x[...], up_w[rows, columns], preferred_element_type=jnp.float32)
        if last:
            out_ref[:, columns] = (gate / (1.0 + jnp.exp(-gate)) * up).astype(jnp.bfloat16)
        else:
            gate_out[:, columns] = gate
            up_out[:, columns] = up
        return carry

    lax.fori_loop(0, gate_w.shape[1] // tile, step, 0)
    finish()


VMEM = pl.BlockSpec(memory_space=pltpu.VMEM)
SMEM = pl.BlockSpec(memory_space=pltpu.SMEM)
HBM = pl.BlockSpec(memory_space=pltpu.HBM)


def first_weights(where, pieces, after, w_gate, w_up, depth):
    width = w_gate.shape[2]
    return pl.pallas_call(
        functools.partial(first_kernel, pieces),
        in_specs=[SMEM, HBM, HBM, HBM],
        out_specs=[VMEM] * 2,
        out_shape=[pltpu.VMEM((depth, width), jnp.bfloat16)] * 2,
        scratch_shapes=[pltpu.SemaphoreType.DMA((2, 2 * len(pieces)))],
        compiler_params=pltpu.CompilerParams(vmem_limit_bytes=1 << 20),
        name="first",
    )(where, after, w_gate, w_up)


def gate_up(where, xs, weights, totals, following, w_gate, w_up, w_down):
    rows = xs[0].shape[0]
    depth, width = weights[0].shape
    last = following is None
    if last:
        sources = [w_down]
        out_shape = [pltpu.VMEM((rows, width), jnp.bfloat16)]
        out_shape += [pltpu.VMEM((width // 2, w_down.shape[2] // 2), jnp.bfloat16)] * 2
    else:
        sources = [w_gate, w_up]
        out_shape = [pltpu.VMEM((rows, width), jnp.float32)] * 2
        out_shape += [pltpu.VMEM((depth, width), jnp.bfloat16)] * 2
    plan = (len(xs), totals is None, following, tile_of(width, 512))
    totals = totals or []
    at = 1 + len(xs) + 2
    return pl.pallas_call(
        functools.partial(gate_up_kernel, plan),
        in_specs=[SMEM] + [VMEM] * (len(xs) + 2 + len(totals)) + [HBM] * len(sources),
        out_specs=[VMEM] * len(out_shape),
        out_shape=out_shape,
        scratch_shapes=[pltpu.SemaphoreType.DMA((2, max(4, DOWN_PARTS)))],
        input_output_aliases={} if last or not totals else {at + i: i for i in range(2)},
        compiler_params=pltpu.CompilerParams(vmem_limit_bytes=8 << 20),
        cost_estimate=pl.CostEstimate(
            flops=4 * rows * depth * width, transcendentals=0, bytes_accessed=4 * depth * width
        ),
    )(where, *xs, *weights, *totals, *sources)


def down_kernel(plan, where_ref, h_ref, w_a, w_b, after_ref, *refs):
    c, part, tile, columns = plan
    here = where_ref[0]
    if part is None:
        keep_ref, send_ref, token_ref = refs
        finish = None
    else:
        w_down, keep_ref, send_ref, token_ref, next_ref, sems = refs
        finish = run_copies(down_copies(0, (part,), here, w_down, (next_ref,), sems))
    quarter = columns * OUT_CHUNKS
    half = w_a.shape[0]
    for p, out_ref in enumerate((keep_ref, send_ref)):
        start = ((here & 1) ^ p) * quarter + c * columns
        for j in range(columns // tile):
            at = pl.ds(pl.multiple_of(start + j * tile, tile), tile)
            total = jnp.dot(h_ref[:, :half], w_a[:, at], preferred_element_type=jnp.float32)
            total = total + jnp.dot(
                h_ref[:, half:], w_b[:, at], preferred_element_type=jnp.float32
            )
            out_ref[:, j * tile : (j + 1) * tile] = total.astype(out_ref.dtype)
    token_ref[...] = jnp.zeros_like(token_ref)
    if finish is not None:
        finish()


def down(where, c, h, weights, after, part, w_down):
    rows, depth = h.shape
    half, both = weights[0].shape
    columns = both // 2 // OUT_CHUNKS
    out_shape = [
        pltpu.VMEM((rows, columns), jnp.float32),
        pltpu.VMEM((rows, columns), jnp.bfloat16),
        jax.ShapeDtypeStruct((8, LANES), jnp.float32),
    ]
    more = part is not None
    if more:
        out_shape.append(pltpu.VMEM((half, both), jnp.bfloat16))
    return pl.pallas_call(
        functools.partial(down_kernel, (c, part, tile_of(columns, 512), columns)),
        in_specs=[SMEM, VMEM, VMEM, VMEM, HBM] + [HBM] * more,
        out_specs=[VMEM] * len(out_shape),
        out_shape=out_shape,
        scratch_shapes=[pltpu.SemaphoreType.DMA((2, DOWN_PARTS))] * more,
        compiler_params=pltpu.CompilerParams(vmem_limit_bytes=8 << 20),
        cost_estimate=pl.CostEstimate(
            flops=4 * rows * depth * columns, transcendentals=0, bytes_accessed=4 * depth * columns
        ),
    )(where, h, *weights, after, *([w_down] * more))


def combine_kernel(combine_ref, *refs):
    parts, out_ref = refs[:-1], refs[-1]
    micro, _, rows = combine_ref.shape
    left = jnp.concatenate([combine_ref[m].T for m in range(micro)], axis=0)
    pieces = []
    for _ in range(3):
        piece = left.astype(jnp.bfloat16)
        pieces.append(piece)
        left = left - piece.astype(jnp.float32)
    pieces = jnp.concatenate(pieces, axis=0)
    each = micro * rows
    for at, part in enumerate(parts):
        width = part.shape[1]
        total = jnp.dot(pieces, part[...], preferred_element_type=jnp.float32)
        total = (total[2 * each :] + total[each : 2 * each]) + total[:each]
        total = total.astype(jnp.bfloat16)
        for m in range(micro):
            out_ref[m, :, at * width : (at + 1) * width] = total[m * rows : (m + 1) * rows]


def local(dp, tensor, tokens, routes, probs, w_gate, w_up, w_down):
    micro, rows, features = tokens.shape
    experts = probs.shape[-1]
    cap2 = micro * CAP
    blocks = features // LANES
    slots_all = dp * cap2
    where = lax.axis_index("tensor")[None]
    w_gate, w_up, w_down = (
        pltpu.with_memory_space_constraint(w, pltpu.HBM) for w in (w_gate, w_up, w_down)
    )
    core = [(t, t ^ 1) for t in range(tensor)]
    row = [(t, t ^ 2) for t in range(tensor)]

    width = features // IN_CHUNKS
    dims = (dp, cap2, experts)
    routes, probs = routes.transpose(0, 2, 1), probs.transpose(0, 2, 1)
    sent = pl.pallas_call(
        functools.partial(tables_kernel, dims),
        out_shape=pltpu.VMEM((dp, blocks * cap2 + experts, LANES), jnp.bfloat16),
        scratch_shapes=[pltpu.VMEM((experts, LANES), jnp.float32)],
        compiler_params=pltpu.CompilerParams(vmem_limit_bytes=24 << 20),
        name="tables",
    )(*(pltpu.with_memory_space_constraint(a, pltpu.HBM) for a in (routes, probs, tokens)))
    arrived = lax.all_to_all(sent, "dp", split_axis=0, concat_axis=0, tiled=True)
    combine = pl.pallas_call(
        functools.partial(weights_kernel, dims),
        out_shape=jax.ShapeDtypeStruct((micro, slots_all, rows), jnp.float32),
        compiler_params=pltpu.CompilerParams(vmem_limit_bytes=8 << 20),
        name="weights",
    )(routes, probs)
    *xs, loss = pl.pallas_call(
        functools.partial(repack_kernel, (dp, cap2, blocks, micro, experts, rows * dp)),
        out_shape=[pltpu.VMEM((slots_all, width), jnp.bfloat16)] * IN_CHUNKS
        + [jax.ShapeDtypeStruct((experts, micro), jnp.float32)],
        compiler_params=pltpu.CompilerParams(vmem_limit_bytes=4 << 20),
        name="repack",
    )(pltpu.with_memory_space_constraint(arrived, pltpu.VMEM))
    paired, crossed = [], []
    for x in xs:
        paired.append(lax.ppermute(x, "tensor", core))
        crossed.append(lax.ppermute(x, "tensor", row))
    chunks = range(IN_CHUNKS)
    stages = [[(q, c) for c in chunks] for q in range(2)] + [[(2, c), (3, c)] for c in chunks]
    operands = [xs, paired]
    for c in chunks:
        operands.append([crossed[c], lax.ppermute(crossed[c], "tensor", core)])
    weights = first_weights(where, stages[0], loss, w_gate, w_up, features)
    totals = None
    for at, pieces in enumerate(operands):
        following = stages[at + 1] if at + 1 < len(stages) else None
        made = gate_up(where, pieces, weights, totals, following, w_gate, w_up, w_down)
        totals, weights = made[:-2], made[-2:]
    hidden = totals[0]

    returned = []
    kept = {}
    width = features // OUT_CHUNKS
    token = loss
    for side in (1, 0):
        upcoming = []
        for c in range(OUT_CHUNKS):
            keep, send, token, *more = down(
                where, c, hidden, weights, token, c if side else None, w_down
            )
            upcoming += more
            kept[side, c] = (keep, lax.ppermute(send, "tensor", core))
        weights = upcoming
    crossed = []
    for c in range(OUT_CHUNKS):
        keep, got = kept[1, c]
        total = (keep + got.astype(jnp.float32)).astype(jnp.bfloat16)
        crossed.append(lax.ppermute(total, "tensor", row))
    for c in range(OUT_CHUNKS):
        keep, got = kept[0, c]
        total = keep + got.astype(jnp.float32) + crossed[c].astype(jnp.float32)
        total = total.astype(jnp.bfloat16).reshape(dp, cap2, width)
        back = lax.all_to_all(total, "dp", split_axis=0, concat_axis=0, tiled=True)
        back = pltpu.with_memory_space_constraint(back.reshape(slots_all, width), pltpu.VMEM)
        returned.append(back)
    mixed = pl.pallas_call(
        combine_kernel,
        out_shape=jax.ShapeDtypeStruct((micro, rows, features), jnp.bfloat16),
        compiler_params=pltpu.CompilerParams(vmem_limit_bytes=16 << 20),
        name="combine",
    )(combine, *returned)
    return mixed, loss.T


def solution(mesh):
    dp, tensor = mesh.shape["dp"], mesh.shape["tensor"]
    in_specs = (
        P(None, "dp", "tensor"),
        P(None, "dp", None),
        P(None, "dp", None),
        P("dp", None, "tensor"),
        P("dp", None, "tensor"),
        P("dp", "tensor", None),
    )
    out_specs = (P(None, "dp", "tensor"), P())


    def body(*args):
        return local(dp, tensor, *args)

    return jax.shard_map(
        body, mesh=mesh, in_specs=in_specs, out_specs=out_specs, check_vma=False
    )
```

```python
import functools

import jax
import jax.numpy as jnp
from jax import lax
from jax.experimental import pallas as pl
from jax.experimental.pallas import tpu as pltpu
from jax.sharding import PartitionSpec as P


CAP = 20
LANES = 128
PAIR_KEY = 64
IN_CHUNKS = 2
OUT_CHUNKS = 2
DOWN_PARTS = 1


def tile_of(size, most):
    return max(d for d in range(LANES, max(most, LANES) + 1, LANES) if size % d == 0)


def block_device(dims, rows, first):
    dp, cap2, _ = dims
    device = lax.broadcasted_iota(jnp.int32, (dp * cap2, rows), 0).astype(jnp.float32)
    device = jnp.floor((device + 0.5) * (1.0 / cap2))
    if first is None:
        return device
    device = device + first.astype(jnp.float32)
    return device - jnp.floor((device + 0.5) * (1.0 / dp)) * dp


def places(dims, device, routes_ref, m):
    dp, cap2, experts = dims
    rows = routes_ref.shape[2]
    at = lax.broadcasted_iota(jnp.int32, (dp * cap2, rows), 0).astype(jnp.float32)
    at = at - jnp.floor((at + 0.5) * (1.0 / cap2)) * cap2
    keys = jnp.floor((device + 0.5) * (experts / dp)) * PAIR_KEY + at
    earlier = lax.broadcasted_iota(jnp.int32, (rows, rows), 0) < lax.broadcasted_iota(
        jnp.int32, (rows, rows), 1
    )
    ids = lax.broadcasted_iota(jnp.int32, (experts, rows), 0)
    route = routes_ref[m]
    hits = [(route[k : k + 1, :] == ids).astype(jnp.float32) for k in range(2)]
    named = hits[0] + hits[1]
    before = jnp.dot(named, earlier.astype(jnp.float32), preferred_element_type=jnp.float32)
    here = []
    for k in range(2):
        place = jnp.sum(before * hits[k], axis=0, keepdims=True)
        own_key = route[k : k + 1, :].astype(jnp.float32) * PAIR_KEY + (m * CAP + place)
        here.append((keys == own_key).astype(jnp.float32))
    return hits, named, here


def tables_kernel(dims, where_ref, routes_ref, probs_ref, tokens_ref, *refs):
    dp, cap2, experts = dims
    sent, aux_ref = refs[:dp], refs[dp]
    device = block_device(dims, routes_ref.shape[2], where_ref[0])
    micro = routes_ref.shape[0]
    blocks = tokens_ref.shape[2] // LANES
    aux_ref[...] = jnp.zeros_like(aux_ref)
    slots = jnp.zeros((dp * cap2, tokens_ref.shape[2]), jnp.float32)
    for m in range(micro):
        _, named, here = places(dims, device, routes_ref, m)
        pick = (here[0] + here[1]).astype(jnp.bfloat16)
        slots = slots + jnp.dot(pick, tokens_ref[m], preferred_element_type=jnp.float32)
        sums = jnp.sum(probs_ref[m], axis=1, keepdims=True)
        aux_ref[0:experts, m : m + 1] = jnp.sum(named, axis=1, keepdims=True)
        for piece in range(3):
            part = sums.astype(jnp.bfloat16).astype(jnp.float32)
            column = (piece + 1) * micro + m
            aux_ref[0:experts, column : column + 1] = part
            sums = sums - part
    slots = slots.astype(jnp.bfloat16)
    aux = aux_ref[...].astype(jnp.bfloat16)
    for d in range(dp):
        for b in range(blocks):
            sent[d][b * cap2 : (b + 1) * cap2, :] = slots[
                d * cap2 : (d + 1) * cap2, b * LANES : (b + 1) * LANES
            ]
        sent[d][blocks * cap2 :, :] = aux


def weights_kernel(dims, where_ref, routes_ref, probs_ref, *orders):
    dp, cap2, experts = dims
    micro, _, rows = routes_ref.shape
    for shifted, pieces_ref in enumerate(orders):
        device = block_device(dims, rows, where_ref[0] if shifted else None)
        for m in range(micro):
            hits, _, here = places(dims, device, routes_ref, m)
            picked = [jnp.sum(probs_ref[m] * hit, axis=0, keepdims=True) for hit in hits]
            total = picked[0] + picked[1]
            left = (here[0] * (picked[0] / total) + here[1] * (picked[1] / total)).T
            for piece in range(3):
                part = left.astype(jnp.bfloat16)
                at = (piece * micro + m) * rows
                pieces_ref[at : at + rows, :] = part
                left = left - part.astype(jnp.float32)


def repack_kernel(dims, where_ref, *refs):
    dp, blocks, tokens_all, count = dims
    arrived, refs = refs[:dp], refs[dp:]
    xs, loss_ref, aux_ref = refs[:count], refs[count], refs[count + 1]
    experts, micro = loss_ref.shape
    cap2 = xs[0].shape[1]
    per = blocks // count
    for shift in range(dp):
        group = lax.rem(where_ref[0] + (dp - shift), dp)
        for b in range(blocks):
            xs[b // per][group, :, b % per * LANES : (b % per + 1) * LANES] = arrived[shift][
                b * cap2 : (b + 1) * cap2, :
            ]
        aux_ref[group] = arrived[shift][blocks * cap2 :, :].astype(jnp.float32)
    total = jnp.zeros((experts, LANES), jnp.float32)
    for group in range(dp):
        total = total + aux_ref[group]
    count = total[:, 0:micro]
    prob = total[:, 3 * micro : 4 * micro] + total[:, 2 * micro : 3 * micro]
    prob = prob + total[:, micro : 2 * micro]
    loss_ref[...] = experts * (count / (tokens_all * 2)) * (prob / tokens_all)


def gate_up_copies(pieces, here, sources, targets, sems):
    copies = []
    depth = targets[0].shape[0] // len(pieces)
    half = depth // 2
    for i, (quarter, c) in enumerate(pieces):
        start = ((here ^ quarter) * IN_CHUNKS + c) * depth
        for k, (source, target) in enumerate(zip(sources, targets)):
            for part in range(2):
                at = pl.multiple_of(start + part * half, half)
                copies.append(
                    pltpu.make_async_copy(
                        source.at[0, pl.ds(at, half), :],
                        target.at[pl.ds(i * depth + part * half, half), :],
                        sems.at[k, 2 * i + part],
                    )
                )
    return copies


def down_copies(side, parts, here, source, targets, sems):
    copies = []
    half, columns = targets[0].shape
    at = pl.multiple_of(((here >> 1) ^ side) * columns, columns)
    step = half // DOWN_PARTS
    for i, target in zip(parts, targets):
        for part in range(DOWN_PARTS):
            copies.append(
                pltpu.make_async_copy(
                    source.at[0, pl.ds(i * half + part * step, step), pl.ds(at, columns)],
                    target.at[pl.ds(part * step, step), :],
                    sems.at[i, part],
                )
            )
    return copies


def run_copies(copies):
    for copy in copies:
        copy.start()

    def finish():
        for copy in copies:
            copy.wait()

    return finish


def first_kernel(pieces, where_ref, after_ref, w_gate, w_up, gate_ref, up_ref, sems):
    sources, targets = (w_gate, w_up), (gate_ref, up_ref)
    run_copies(gate_up_copies(pieces, where_ref[0], sources, targets, sems))()


def gate_up_kernel(plan, where_ref, *refs):
    count, first, following, tile = plan
    last = following is None
    xs, refs = refs[:count], refs[count:]
    gate_w, up_w, refs = refs[0], refs[1], refs[2:]
    if not first:
        gate_in, up_in, refs = refs[0], refs[1], refs[2:]
    here = where_ref[0]
    if last:
        w_down, out_ref, next_a, next_b, sems = refs
        copies = down_copies(1, (0, 1), here, w_down, (next_a, next_b), sems)
    else:
        w_gate, w_up, gate_out, up_out, next_a, next_b, sems = refs
        copies = gate_up_copies(following, here, (w_gate, w_up), (next_a, next_b), sems)
    finish = run_copies(copies)
    depth = gate_w.shape[0] // count

    def step(j, carry):
        columns = pl.ds(pl.multiple_of(j * tile, tile), tile)
        if first:
            gate = up = 0.0
        else:
            gate, up = gate_in[:, columns], up_in[:, columns]
        for i, x in enumerate(xs):
            rows = slice(i * depth, (i + 1) * depth)
            gate = gate + jnp.dot(
                x[...], gate_w[rows, columns], preferred_element_type=jnp.float32
            )
            up = up + jnp.dot(x[...], up_w[rows, columns], preferred_element_type=jnp.float32)
        if last:
            out_ref[:, columns] = (gate / (1.0 + jnp.exp(-gate)) * up).astype(jnp.bfloat16)
        else:
            gate_out[:, columns] = gate
            up_out[:, columns] = up
        return carry

    lax.fori_loop(0, gate_w.shape[1] // tile, step, 0)
    finish()


VMEM = pl.BlockSpec(memory_space=pltpu.VMEM)
SMEM = pl.BlockSpec(memory_space=pltpu.SMEM)
HBM = pl.BlockSpec(memory_space=pltpu.HBM)


def first_weights(where, pieces, after, w_gate, w_up, depth):
    width = w_gate.shape[2]
    return pl.pallas_call(
        functools.partial(first_kernel, pieces),
        in_specs=[SMEM, pl.BlockSpec(memory_space=pl.ANY), HBM, HBM],
        out_specs=[VMEM] * 2,
        out_shape=[pltpu.VMEM((depth, width), jnp.bfloat16)] * 2,
        scratch_shapes=[pltpu.SemaphoreType.DMA((2, 2 * len(pieces)))],
        compiler_params=pltpu.CompilerParams(vmem_limit_bytes=1 << 20),
        name="first",
    )(where, after, w_gate, w_up)


def gate_up(where, xs, weights, totals, following, w_gate, w_up, w_down):
    rows = xs[0].shape[0]
    depth, width = weights[0].shape
    last = following is None
    if last:
        sources = [w_down]
        out_shape = [pltpu.VMEM((rows, width), jnp.bfloat16)]
        out_shape += [pltpu.VMEM((width // 2, w_down.shape[2] // 2), jnp.bfloat16)] * 2
    else:
        sources = [w_gate, w_up]
        out_shape = [pltpu.VMEM((rows, width), jnp.float32)] * 2
        out_shape += [pltpu.VMEM((depth, width), jnp.bfloat16)] * 2
    plan = (len(xs), totals is None, following, tile_of(width, (5 << 20) // (8 * rows)))
    totals = totals or []
    at = 1 + len(xs) + 2
    return pl.pallas_call(
        functools.partial(gate_up_kernel, plan),
        in_specs=[SMEM] + [VMEM] * (len(xs) + 2 + len(totals)) + [HBM] * len(sources),
        out_specs=[VMEM] * len(out_shape),
        out_shape=out_shape,
        scratch_shapes=[pltpu.SemaphoreType.DMA((2, max(4, DOWN_PARTS)))],
        input_output_aliases={} if last or not totals else {at + i: i for i in range(2)},
        compiler_params=pltpu.CompilerParams(vmem_limit_bytes=8 << 20),
        cost_estimate=pl.CostEstimate(
            flops=4 * rows * depth * width, transcendentals=0, bytes_accessed=4 * depth * width
        ),
    )(where, *xs, *weights, *totals, *sources)


def down_kernel(plan, where_ref, h_ref, w_a, w_b, after_ref, *refs):
    c, part, tile, columns = plan
    here = where_ref[0]
    if part is None:
        keep_ref, send_ref, token_ref = refs
        finish = None
    else:
        w_down, keep_ref, send_ref, token_ref, next_ref, sems = refs
        finish = run_copies(down_copies(0, (part,), here, w_down, (next_ref,), sems))
    quarter = columns * OUT_CHUNKS
    half = w_a.shape[0]

    def step(j, carry):
        for p, out_ref in enumerate((keep_ref, send_ref)):
            start = ((here & 1) ^ p) * quarter + c * columns
            at = pl.ds(pl.multiple_of(start + j * tile, tile), tile)
            total = jnp.dot(h_ref[:, :half], w_a[:, at], preferred_element_type=jnp.float32)
            total = total + jnp.dot(
                h_ref[:, half:], w_b[:, at], preferred_element_type=jnp.float32
            )
            out_ref[:, pl.ds(pl.multiple_of(j * tile, tile), tile)] = total.astype(out_ref.dtype)
        return carry

    lax.fori_loop(0, columns // tile, step, 0)
    token_ref[...] = jnp.zeros_like(token_ref)
    if finish is not None:
        finish()


def down(where, c, h, weights, after, part, w_down):
    rows, depth = h.shape
    half, both = weights[0].shape
    columns = both // 2 // OUT_CHUNKS
    out_shape = [
        pltpu.VMEM((rows, columns), jnp.float32),
        pltpu.VMEM((rows, columns), jnp.bfloat16),
        jax.ShapeDtypeStruct((8, LANES), jnp.float32),
    ]
    more = part is not None
    if more:
        out_shape.append(pltpu.VMEM((half, both), jnp.bfloat16))
    return pl.pallas_call(
        functools.partial(down_kernel, (c, part, tile_of(columns, 256), columns)),
        in_specs=[SMEM, VMEM, VMEM, VMEM, HBM] + [HBM] * more,
        out_specs=[VMEM] * len(out_shape),
        out_shape=out_shape,
        scratch_shapes=[pltpu.SemaphoreType.DMA((2, DOWN_PARTS))] * more,
        compiler_params=pltpu.CompilerParams(vmem_limit_bytes=8 << 20),
        cost_estimate=pl.CostEstimate(
            flops=4 * rows * depth * columns, transcendentals=0, bytes_accessed=4 * depth * columns
        ),
    )(where, h, *weights, after, *([w_down] * more))


def spread_kernel(dp, where_ref, keep_ref, got_ref, crossed_ref, *outs):
    for shift in range(dp):
        group = lax.rem(where_ref[0] + (dp - shift), dp)
        total = keep_ref[group] + got_ref[group].astype(jnp.float32)
        total = total + crossed_ref[group].astype(jnp.float32)
        outs[shift][...] = total.astype(jnp.bfloat16)


def combine_kernel(whole_ref, shifted_ref, first_ref, *refs):
    blocks, out_ref, rows_ref = refs[:-2], refs[-2], refs[-1]
    micro, rows, _ = out_ref.shape
    each = micro * rows
    cap2 = blocks[0].shape[0]
    for shift, block in enumerate(blocks):
        rows_ref[shift * cap2 : (shift + 1) * cap2, :] = block[...]
    at = 0
    for pieces, part in ((whole_ref, first_ref), (shifted_ref, rows_ref)):
        width = part.shape[1]
        total = jnp.dot(pieces[...], part[...], preferred_element_type=jnp.float32)
        total = (total[2 * each :] + total[each : 2 * each]) + total[:each]
        total = total.astype(jnp.bfloat16)
        for m in range(micro):
            out_ref[m, :, at : at + width] = total[m * rows : (m + 1) * rows]
        at += width


def local(dp, tensor, tokens, routes, probs, w_gate, w_up, w_down):
    micro, rows, features = tokens.shape
    experts = probs.shape[-1]
    cap2 = micro * CAP
    blocks = features // LANES
    slots_all = dp * cap2
    where = lax.axis_index("tensor")[None]
    w_gate, w_up, w_down = (
        pltpu.with_memory_space_constraint(w, pltpu.HBM) for w in (w_gate, w_up, w_down)
    )
    core = [(t, t ^ 1) for t in range(tensor)]
    row = [(t, t ^ 2) for t in range(tensor)]

    width = features // IN_CHUNKS
    dims = (dp, cap2, experts)
    routes, probs = routes.transpose(0, 2, 1), probs.transpose(0, 2, 1)
    place = lax.axis_index("dp")[None]
    inputs = (pltpu.with_memory_space_constraint(a, pltpu.HBM) for a in (routes, probs, tokens))
    sent = pl.pallas_call(
        functools.partial(tables_kernel, dims),
        in_specs=[SMEM] + [VMEM] * 3,
        out_shape=[pltpu.VMEM((blocks * cap2 + experts, LANES), jnp.bfloat16)] * dp,
        scratch_shapes=[pltpu.VMEM((experts, LANES), jnp.float32)],
        compiler_params=pltpu.CompilerParams(vmem_limit_bytes=48 << 20),
        name="tables",
    )(place, *inputs)
    arrived = [sent[0]]
    for shift in range(1, dp):
        onward = [(i, (i + shift) % dp) for i in range(dp)]
        arrived.append(lax.ppermute(sent[shift], "dp", onward))
    combine = pl.pallas_call(
        functools.partial(weights_kernel, dims),
        in_specs=[SMEM] + [VMEM] * 2,
        out_shape=[jax.ShapeDtypeStruct((3 * micro * rows, slots_all), jnp.bfloat16)] * 2,
        compiler_params=pltpu.CompilerParams(vmem_limit_bytes=8 << 20),
        name="weights",
    )(place, routes, probs)
    chunks = range(IN_CHUNKS)
    stages = [[(q, c) for c in chunks] for q in range(2)] + [[(2, c), (3, c)] for c in chunks]
    weights = first_weights(where, stages[0], sent[0], w_gate, w_up, features)
    *xs, loss = pl.pallas_call(
        functools.partial(repack_kernel, (dp, blocks, rows * dp, IN_CHUNKS)),
        in_specs=[SMEM] + [VMEM] * dp,
        out_shape=[pltpu.VMEM((dp, cap2, width), jnp.bfloat16)] * IN_CHUNKS
        + [jax.ShapeDtypeStruct((experts, micro), jnp.float32)],
        scratch_shapes=[pltpu.VMEM((dp, experts, LANES), jnp.float32)],
        compiler_params=pltpu.CompilerParams(vmem_limit_bytes=12 << 20),
        name="repack",
    )(place, *arrived)
    xs = [x.reshape(slots_all, width) for x in xs]
    paired, crossed = [], []
    for x in xs:
        paired.append(lax.ppermute(x, "tensor", core))
        crossed.append(lax.ppermute(x, "tensor", row))
    operands = [xs, paired]
    for c in chunks:
        operands.append([crossed[c], lax.ppermute(crossed[c], "tensor", core)])
    totals = None
    for at, pieces in enumerate(operands):
        following = stages[at + 1] if at + 1 < len(stages) else None
        made = gate_up(where, pieces, weights, totals, following, w_gate, w_up, w_down)
        totals, weights = made[:-2], made[-2:]
    hidden = totals[0]

    returned = []
    kept = {}
    width = features // OUT_CHUNKS
    token = loss
    for side in (1, 0):
        upcoming = []
        for c in range(OUT_CHUNKS):
            keep, send, token, *more = down(
                where, c, hidden, weights, token, c if side else None, w_down
            )
            upcoming += more
            kept[side, c] = (keep, lax.ppermute(send, "tensor", core))
        weights = upcoming
    crossed = []
    for c in range(OUT_CHUNKS):
        keep, got = kept[1, c]
        total = (keep + got.astype(jnp.float32)).astype(jnp.bfloat16)
        crossed.append(lax.ppermute(total, "tensor", row))
    keep, got = kept[0, 0]
    total = keep + got.astype(jnp.float32) + crossed[0].astype(jnp.float32)
    total = total.astype(jnp.bfloat16).reshape(dp, cap2, width)
    back = lax.all_to_all(total, "dp", split_axis=0, concat_axis=0, tiled=True)
    returned.append(
        pltpu.with_memory_space_constraint(back.reshape(slots_all, width), pltpu.VMEM)
    )
    blocks = pl.pallas_call(
        functools.partial(spread_kernel, dp),
        in_specs=[SMEM] + [VMEM] * 3,
        out_shape=[jax.ShapeDtypeStruct((cap2, width), jnp.bfloat16)] * dp,
        compiler_params=pltpu.CompilerParams(vmem_limit_bytes=12 << 20),
        name="spread",
    )(place, *(a.reshape(dp, cap2, width) for a in (*kept[0, 1], crossed[1])))
    returned.append(blocks[0])
    for shift in range(1, dp):
        home = [(i, (i - shift) % dp) for i in range(dp)]
        returned.append(lax.ppermute(blocks[shift], "dp", home))
    mixed = pl.pallas_call(
        combine_kernel,
        out_shape=jax.ShapeDtypeStruct((micro, rows, features), jnp.bfloat16),
        scratch_shapes=[pltpu.VMEM((slots_all, width), jnp.bfloat16)],
        compiler_params=pltpu.CompilerParams(vmem_limit_bytes=16 << 20),
        name="combine",
    )(*combine, *returned)
    return mixed, loss.T


def solution(mesh):
    dp, tensor = mesh.shape["dp"], mesh.shape["tensor"]
    in_specs = (
        P(None, "dp", "tensor"),
        P(None, "dp", None),
        P(None, "dp", None),
        P("dp", None, "tensor"),
        P("dp", None, "tensor"),
        P("dp", "tensor", None),
    )
    out_specs = (P(None, "dp", "tensor"), P())


    def body(*args):
        return local(dp, tensor, *args)

    return jax.shard_map(
        body, mesh=mesh, in_specs=in_specs, out_specs=out_specs, check_vma=False
    )
```

```python
import functools

import jax
import jax.numpy as jnp
from jax import lax
from jax.experimental import pallas as pl
from jax.experimental.pallas import tpu as pltpu
from jax.sharding import PartitionSpec as P


CAP = 20
LANES = 128
PAIR_KEY = 64
IN_CHUNKS = 2
OUT_CHUNKS = 2
DOWN_PARTS = 1


def tile_of(size, most):
    return max(d for d in range(LANES, max(most, LANES) + 1, LANES) if size % d == 0)


def block_device(dims, rows, first):
    dp, cap2, _ = dims
    device = lax.broadcasted_iota(jnp.int32, (dp * cap2, rows), 0).astype(jnp.float32)
    device = jnp.floor((device + 0.5) * (1.0 / cap2))
    if first is None:
        return device
    return (device.astype(jnp.int32) ^ first).astype(jnp.float32)


def places(dims, device, routes_ref, m):
    dp, cap2, experts = dims
    rows = routes_ref.shape[2]
    at = lax.broadcasted_iota(jnp.int32, (dp * cap2, rows), 0).astype(jnp.float32)
    at = at - jnp.floor((at + 0.5) * (1.0 / cap2)) * cap2
    keys = jnp.floor((device + 0.5) * (experts / dp)) * PAIR_KEY + at
    earlier = lax.broadcasted_iota(jnp.int32, (rows, rows), 0) < lax.broadcasted_iota(
        jnp.int32, (rows, rows), 1
    )
    ids = lax.broadcasted_iota(jnp.int32, (experts, rows), 0)
    route = routes_ref[m]
    hits = [(route[k : k + 1, :] == ids).astype(jnp.float32) for k in range(2)]
    named = hits[0] + hits[1]
    before = jnp.dot(named, earlier.astype(jnp.float32), preferred_element_type=jnp.float32)
    here = []
    for k in range(2):
        place = jnp.sum(before * hits[k], axis=0, keepdims=True)
        own_key = route[k : k + 1, :].astype(jnp.float32) * PAIR_KEY + (m * CAP + place)
        here.append((keys == own_key).astype(jnp.float32))
    return hits, named, here


def tables_kernel(dims, where_ref, routes_ref, probs_ref, tokens_ref, *refs):
    dp, cap2, experts = dims
    sent, aux_ref = refs[:dp], refs[dp]
    device = block_device(dims, routes_ref.shape[2], where_ref[0])
    micro = routes_ref.shape[0]
    blocks = tokens_ref.shape[2] // LANES
    aux_ref[...] = jnp.zeros_like(aux_ref)
    slots = jnp.zeros((dp * cap2, tokens_ref.shape[2]), jnp.float32)
    for m in range(micro):
        _, named, here = places(dims, device, routes_ref, m)
        pick = (here[0] + here[1]).astype(jnp.bfloat16)
        slots = slots + jnp.dot(pick, tokens_ref[m], preferred_element_type=jnp.float32)
        sums = jnp.sum(probs_ref[m], axis=1, keepdims=True)
        aux_ref[0:experts, m : m + 1] = jnp.sum(named, axis=1, keepdims=True)
        for piece in range(3):
            part = sums.astype(jnp.bfloat16).astype(jnp.float32)
            column = (piece + 1) * micro + m
            aux_ref[0:experts, column : column + 1] = part
            sums = sums - part
    slots = slots.astype(jnp.bfloat16)
    aux = aux_ref[...].astype(jnp.bfloat16)
    for d in range(dp):
        for b in range(blocks):
            sent[d][b * cap2 : (b + 1) * cap2, :] = slots[
                d * cap2 : (d + 1) * cap2, b * LANES : (b + 1) * LANES
            ]
        sent[d][blocks * cap2 :, :] = aux


def weights_kernel(dims, where_ref, routes_ref, probs_ref, after_ref, *orders):
    dp, cap2, experts = dims
    micro, _, rows = routes_ref.shape
    for shifted, pieces_ref in enumerate(orders):
        device = block_device(dims, rows, where_ref[0] if shifted else None)
        for m in range(micro):
            hits, _, here = places(dims, device, routes_ref, m)
            picked = [jnp.sum(probs_ref[m] * hit, axis=0, keepdims=True) for hit in hits]
            total = picked[0] + picked[1]
            left = (here[0] * (picked[0] / total) + here[1] * (picked[1] / total)).T
            for piece in range(3):
                part = left.astype(jnp.bfloat16)
                at = (piece * micro + m) * rows
                pieces_ref[at : at + rows, :] = part
                left = left - part.astype(jnp.float32)


def repack_kernel(dims, where_ref, *refs):
    dp, blocks, tokens_all, count = dims
    arrived, refs = refs[:dp], refs[dp:]
    xs, loss_ref, aux_ref = refs[:count], refs[count], refs[count + 1]
    experts, micro = loss_ref.shape
    cap2 = xs[0].shape[1]
    per = blocks // count
    for shift in range(dp):
        group = where_ref[0] ^ shift
        for b in range(blocks):
            xs[b // per][group, :, b % per * LANES : (b % per + 1) * LANES] = arrived[shift][
                b * cap2 : (b + 1) * cap2, :
            ]
        aux_ref[group] = arrived[shift][blocks * cap2 :, :].astype(jnp.float32)
    total = jnp.zeros((experts, LANES), jnp.float32)
    for group in range(dp):
        total = total + aux_ref[group]
    count = total[:, 0:micro]
    prob = total[:, 3 * micro : 4 * micro] + total[:, 2 * micro : 3 * micro]
    prob = prob + total[:, micro : 2 * micro]
    loss_ref[...] = experts * (count / (tokens_all * 2)) * (prob / tokens_all)


def gate_up_copies(pieces, here, sources, targets, sems):
    copies = []
    depth = targets[0].shape[0] // len(pieces)
    half = depth // 2
    for i, (quarter, c) in enumerate(pieces):
        start = ((here ^ quarter) * IN_CHUNKS + c) * depth
        for k, (source, target) in enumerate(zip(sources, targets)):
            for part in range(2):
                at = pl.multiple_of(start + part * half, half)
                copies.append(
                    pltpu.make_async_copy(
                        source.at[0, pl.ds(at, half), :],
                        target.at[pl.ds(i * depth + part * half, half), :],
                        sems.at[k, 2 * i + part],
                    )
                )
    return copies


def down_copies(side, parts, here, source, targets, sems):
    copies = []
    half, columns = targets[0].shape
    at = pl.multiple_of(((here >> 1) ^ side) * columns, columns)
    step = half // DOWN_PARTS
    for i, target in zip(parts, targets):
        for part in range(DOWN_PARTS):
            copies.append(
                pltpu.make_async_copy(
                    source.at[0, pl.ds(i * half + part * step, step), pl.ds(at, columns)],
                    target.at[pl.ds(part * step, step), :],
                    sems.at[i, part],
                )
            )
    return copies


def run_copies(copies):
    for copy in copies:
        copy.start()

    def finish():
        for copy in copies:
            copy.wait()

    return finish


def first_kernel(pieces, where_ref, after_ref, w_gate, w_up, gate_ref, up_ref, sems):
    sources, targets = (w_gate, w_up), (gate_ref, up_ref)
    run_copies(gate_up_copies(pieces, where_ref[0], sources, targets, sems))()


def gate_up_kernel(plan, where_ref, *refs):
    count, first, following, tile = plan
    last = following is None
    xs, refs = refs[:count], refs[count:]
    gate_w, up_w, refs = refs[0], refs[1], refs[2:]
    if not first:
        gate_in, up_in, refs = refs[0], refs[1], refs[2:]
    here = where_ref[0]
    if last:
        w_down, out_ref, next_a, next_b, sems = refs
        copies = down_copies(1, (0, 1), here, w_down, (next_a, next_b), sems)
    else:
        w_gate, w_up, gate_out, up_out, next_a, next_b, sems = refs
        copies = gate_up_copies(following, here, (w_gate, w_up), (next_a, next_b), sems)
    finish = run_copies(copies)
    depth = gate_w.shape[0] // count

    def step(j, carry):
        columns = pl.ds(pl.multiple_of(j * tile, tile), tile)
        if first:
            gate = up = 0.0
        else:
            gate, up = gate_in[:, columns], up_in[:, columns]
        for i, x in enumerate(xs):
            rows = slice(i * depth, (i + 1) * depth)
            gate = gate + jnp.dot(
                x[...], gate_w[rows, columns], preferred_element_type=jnp.float32
            )
            up = up + jnp.dot(x[...], up_w[rows, columns], preferred_element_type=jnp.float32)
        if last:
            out_ref[:, columns] = (gate / (1.0 + jnp.exp(-gate)) * up).astype(jnp.bfloat16)
        else:
            gate_out[:, columns] = gate
            up_out[:, columns] = up
        return carry

    lax.fori_loop(0, gate_w.shape[1] // tile, step, 0)
    finish()


VMEM = pl.BlockSpec(memory_space=pltpu.VMEM)
SMEM = pl.BlockSpec(memory_space=pltpu.SMEM)
HBM = pl.BlockSpec(memory_space=pltpu.HBM)


def first_weights(where, pieces, after, w_gate, w_up, depth):
    width = w_gate.shape[2]
    return pl.pallas_call(
        functools.partial(first_kernel, pieces),
        in_specs=[SMEM, pl.BlockSpec(memory_space=pl.ANY), HBM, HBM],
        out_specs=[VMEM] * 2,
        out_shape=[pltpu.VMEM((depth, width), jnp.bfloat16)] * 2,
        scratch_shapes=[pltpu.SemaphoreType.DMA((2, 2 * len(pieces)))],
        compiler_params=pltpu.CompilerParams(vmem_limit_bytes=1 << 20),
        name="first",
    )(where, after, w_gate, w_up)


def gate_up(where, xs, weights, totals, following, w_gate, w_up, w_down):
    rows = xs[0].shape[0]
    depth, width = weights[0].shape
    last = following is None
    if last:
        sources = [w_down]
        out_shape = [pltpu.VMEM((rows, width), jnp.bfloat16)]
        out_shape += [pltpu.VMEM((width // 2, w_down.shape[2] // 2), jnp.bfloat16)] * 2
    else:
        sources = [w_gate, w_up]
        out_shape = [pltpu.VMEM((rows, width), jnp.float32)] * 2
        out_shape += [pltpu.VMEM((depth, width), jnp.bfloat16)] * 2
    plan = (len(xs), totals is None, following, tile_of(width, (5 << 20) // (8 * rows)))
    totals = totals or []
    at = 1 + len(xs) + 2
    return pl.pallas_call(
        functools.partial(gate_up_kernel, plan),
        in_specs=[SMEM] + [VMEM] * (len(xs) + 2 + len(totals)) + [HBM] * len(sources),
        out_specs=[VMEM] * len(out_shape),
        out_shape=out_shape,
        scratch_shapes=[pltpu.SemaphoreType.DMA((2, max(4, DOWN_PARTS)))],
        input_output_aliases={} if last or not totals else {at + i: i for i in range(2)},
        compiler_params=pltpu.CompilerParams(vmem_limit_bytes=8 << 20),
        cost_estimate=pl.CostEstimate(
            flops=4 * rows * depth * width, transcendentals=0, bytes_accessed=4 * depth * width
        ),
    )(where, *xs, *weights, *totals, *sources)


def down_kernel(plan, where_ref, h_ref, w_a, w_b, after_ref, *refs):
    c, part, tile, columns = plan
    here = where_ref[0]
    if part is None:
        keep_ref, send_ref, token_ref = refs
        finish = None
    else:
        w_down, keep_ref, send_ref, token_ref, next_ref, sems = refs
        finish = run_copies(down_copies(0, (part,), here, w_down, (next_ref,), sems))
    quarter = columns * OUT_CHUNKS
    half = w_a.shape[0]

    def step(j, carry):
        for p, out_ref in enumerate((keep_ref, send_ref)):
            start = ((here & 1) ^ p) * quarter + c * columns
            at = pl.ds(pl.multiple_of(start + j * tile, tile), tile)
            total = jnp.dot(h_ref[:, :half], w_a[:, at], preferred_element_type=jnp.float32)
            total = total + jnp.dot(
                h_ref[:, half:], w_b[:, at], preferred_element_type=jnp.float32
            )
            out_ref[:, pl.ds(pl.multiple_of(j * tile, tile), tile)] = total.astype(out_ref.dtype)
        return carry

    lax.fori_loop(0, columns // tile, step, 0)
    token_ref[...] = jnp.zeros_like(token_ref)
    if finish is not None:
        finish()


def down(where, c, h, weights, after, part, w_down):
    rows, depth = h.shape
    half, both = weights[0].shape
    columns = both // 2 // OUT_CHUNKS
    out_shape = [
        pltpu.VMEM((rows, columns), jnp.float32),
        pltpu.VMEM((rows, columns), jnp.bfloat16),
        jax.ShapeDtypeStruct((8, LANES), jnp.float32),
    ]
    more = part is not None
    if more:
        out_shape.append(pltpu.VMEM((half, both), jnp.bfloat16))
    return pl.pallas_call(
        functools.partial(down_kernel, (c, part, tile_of(columns, 256), columns)),
        in_specs=[SMEM, VMEM, VMEM, VMEM, HBM] + [HBM] * more,
        out_specs=[VMEM] * len(out_shape),
        out_shape=out_shape,
        scratch_shapes=[pltpu.SemaphoreType.DMA((2, DOWN_PARTS))] * more,
        compiler_params=pltpu.CompilerParams(vmem_limit_bytes=8 << 20),
        cost_estimate=pl.CostEstimate(
            flops=4 * rows * depth * columns, transcendentals=0, bytes_accessed=4 * depth * columns
        ),
    )(where, h, *weights, after, *([w_down] * more))


def spread_kernel(dp, where_ref, keep_ref, got_ref, crossed_ref, *outs):
    for shift in range(dp):
        group = where_ref[0] ^ shift
        total = keep_ref[group] + got_ref[group].astype(jnp.float32)
        total = total + crossed_ref[group].astype(jnp.float32)
        outs[shift][...] = total.astype(jnp.bfloat16)


def combine_kernel(whole_ref, shifted_ref, first_ref, *refs):
    blocks, out_ref, rows_ref = refs[:-2], refs[-2], refs[-1]
    micro, rows, _ = out_ref.shape
    each = micro * rows
    cap2 = blocks[0].shape[0]
    for shift, block in enumerate(blocks):
        rows_ref[shift * cap2 : (shift + 1) * cap2, :] = block[...]
    at = 0
    for pieces, part in ((whole_ref, first_ref), (shifted_ref, rows_ref)):
        width = part.shape[1]
        total = jnp.dot(pieces[...], part[...], preferred_element_type=jnp.float32)
        total = (total[2 * each :] + total[each : 2 * each]) + total[:each]
        total = total.astype(jnp.bfloat16)
        for m in range(micro):
            out_ref[m, :, at : at + width] = total[m * rows : (m + 1) * rows]
        at += width


def local(dp, tensor, tokens, routes, probs, w_gate, w_up, w_down):
    micro, rows, features = tokens.shape
    experts = probs.shape[-1]
    cap2 = micro * CAP
    blocks = features // LANES
    slots_all = dp * cap2
    where = lax.axis_index("tensor")[None]
    w_gate, w_up, w_down = (
        pltpu.with_memory_space_constraint(w, pltpu.HBM) for w in (w_gate, w_up, w_down)
    )
    core = [(t, t ^ 1) for t in range(tensor)]
    row = [(t, t ^ 2) for t in range(tensor)]

    width = features // IN_CHUNKS
    dims = (dp, cap2, experts)
    routes, probs = routes.transpose(0, 2, 1), probs.transpose(0, 2, 1)
    place = lax.axis_index("dp")[None]
    inputs = (pltpu.with_memory_space_constraint(a, pltpu.HBM) for a in (routes, probs, tokens))
    sent = pl.pallas_call(
        functools.partial(tables_kernel, dims),
        in_specs=[SMEM] + [VMEM] * 3,
        out_shape=[pltpu.VMEM((blocks * cap2 + experts, LANES), jnp.bfloat16)] * dp,
        scratch_shapes=[pltpu.VMEM((experts, LANES), jnp.float32)],
        compiler_params=pltpu.CompilerParams(vmem_limit_bytes=48 << 20),
        name="tables",
    )(place, *inputs)
    arrived = [sent[0]] * dp
    for shift in reversed(range(1, dp)):
        swap = [(i, i ^ shift) for i in range(dp)]
        arrived[shift] = lax.ppermute(sent[shift], "dp", swap)
    chunks = range(IN_CHUNKS)
    stages = [[(q, c) for c in chunks] for q in range(2)] + [[(2, c), (3, c)] for c in chunks]
    weights = first_weights(where, stages[0], sent[0], w_gate, w_up, features)
    *xs, loss = pl.pallas_call(
        functools.partial(repack_kernel, (dp, blocks, rows * dp, IN_CHUNKS)),
        in_specs=[SMEM] + [VMEM] * dp,
        out_shape=[pltpu.VMEM((dp, cap2, width), jnp.bfloat16)] * IN_CHUNKS
        + [jax.ShapeDtypeStruct((experts, micro), jnp.float32)],
        scratch_shapes=[pltpu.VMEM((dp, experts, LANES), jnp.float32)],
        compiler_params=pltpu.CompilerParams(vmem_limit_bytes=12 << 20),
        name="repack",
    )(place, *arrived)
    xs = [x.reshape(slots_all, width) for x in xs]
    paired, crossed = [], []
    for x in xs:
        paired.append(lax.ppermute(x, "tensor", core))
        crossed.append(lax.ppermute(x, "tensor", row))
    operands = [xs, paired]
    for c in chunks:
        operands.append([crossed[c], lax.ppermute(crossed[c], "tensor", core)])
    totals = None
    for at, pieces in enumerate(operands):
        following = stages[at + 1] if at + 1 < len(stages) else None
        made = gate_up(where, pieces, weights, totals, following, w_gate, w_up, w_down)
        totals, weights = made[:-2], made[-2:]
    hidden = totals[0]

    returned = []
    kept = {}
    width = features // OUT_CHUNKS
    token = loss
    for side in (1, 0):
        upcoming = []
        for c in range(OUT_CHUNKS):
            keep, send, token, *more = down(
                where, c, hidden, weights, token, c if side else None, w_down
            )
            upcoming += more
            kept[side, c] = (keep, lax.ppermute(send, "tensor", core))
        weights = upcoming
    combine = pl.pallas_call(
        functools.partial(weights_kernel, dims),
        in_specs=[SMEM] + [VMEM] * 2 + [pl.BlockSpec(memory_space=pl.ANY)],
        out_shape=[jax.ShapeDtypeStruct((3 * micro * rows, slots_all), jnp.bfloat16)] * 2,
        compiler_params=pltpu.CompilerParams(vmem_limit_bytes=8 << 20),
        name="weights",
    )(place, routes, probs, token)
    crossed = []
    for c in range(OUT_CHUNKS):
        keep, got = kept[1, c]
        total = (keep + got.astype(jnp.float32)).astype(jnp.bfloat16)
        crossed.append(lax.ppermute(total, "tensor", row))
    keep, got = kept[0, 0]
    total = keep + got.astype(jnp.float32) + crossed[0].astype(jnp.float32)
    total = total.astype(jnp.bfloat16).reshape(dp, cap2, width)
    back = lax.all_to_all(total, "dp", split_axis=0, concat_axis=0, tiled=True)
    returned.append(
        pltpu.with_memory_space_constraint(back.reshape(slots_all, width), pltpu.VMEM)
    )
    blocks = pl.pallas_call(
        functools.partial(spread_kernel, dp),
        in_specs=[SMEM] + [VMEM] * 3,
        out_shape=[jax.ShapeDtypeStruct((cap2, width), jnp.bfloat16)] * dp,
        compiler_params=pltpu.CompilerParams(vmem_limit_bytes=12 << 20),
        name="spread",
    )(place, *(a.reshape(dp, cap2, width) for a in (*kept[0, 1], crossed[1])))
    home = [blocks[0]] * dp
    for shift in reversed(range(1, dp)):
        swap = [(i, i ^ shift) for i in range(dp)]
        home[shift] = lax.ppermute(blocks[shift], "dp", swap)
    mixed = pl.pallas_call(
        combine_kernel,
        out_shape=jax.ShapeDtypeStruct((micro, rows, features), jnp.bfloat16),
        scratch_shapes=[pltpu.VMEM((slots_all, width), jnp.bfloat16)],
        compiler_params=pltpu.CompilerParams(vmem_limit_bytes=16 << 20),
        name="combine",
    )(*combine, *returned, *home)
    return mixed, loss.T


def solution(mesh):
    dp, tensor = mesh.shape["dp"], mesh.shape["tensor"]
    in_specs = (
        P(None, "dp", "tensor"),
        P(None, "dp", None),
        P(None, "dp", None),
        P("dp", None, "tensor"),
        P("dp", None, "tensor"),
        P("dp", "tensor", None),
    )
    out_specs = (P(None, "dp", "tensor"), P())


    def body(*args):
        return local(dp, tensor, *args)

    return jax.shard_map(
        body, mesh=mesh, in_specs=in_specs, out_specs=out_specs, check_vma=False
    )
```

```python
import functools

import jax
import jax.numpy as jnp
from jax import lax
from jax.experimental import pallas as pl
from jax.experimental.pallas import tpu as pltpu
from jax.sharding import PartitionSpec as P


CAP = 20
LANES = 128
PAIR_KEY = 64
IN_CHUNKS = 2
OUT_CHUNKS = 2
DOWN_PARTS = 1


def tile_of(size, most):
    return max(d for d in range(LANES, max(most, LANES) + 1, LANES) if size % d == 0)


def block_device(dims, rows, first):
    dp, cap2, _ = dims
    device = lax.broadcasted_iota(jnp.int32, (dp * cap2, rows), 0).astype(jnp.float32)
    device = jnp.floor((device + 0.5) * (1.0 / cap2))
    if first is None:
        return device
    return (device.astype(jnp.int32) ^ first).astype(jnp.float32)


def places(dims, device, routes_ref, m):
    dp, cap2, experts = dims
    rows = routes_ref.shape[2]
    at = lax.broadcasted_iota(jnp.int32, (dp * cap2, rows), 0).astype(jnp.float32)
    at = at - jnp.floor((at + 0.5) * (1.0 / cap2)) * cap2
    keys = jnp.floor((device + 0.5) * (experts / dp)) * PAIR_KEY + at
    earlier = lax.broadcasted_iota(jnp.int32, (rows, rows), 0) < lax.broadcasted_iota(
        jnp.int32, (rows, rows), 1
    )
    ids = lax.broadcasted_iota(jnp.int32, (experts, rows), 0)
    route = routes_ref[m]
    hits = [(route[k : k + 1, :] == ids).astype(jnp.float32) for k in range(2)]
    named = hits[0] + hits[1]
    before = jnp.dot(named, earlier.astype(jnp.float32), preferred_element_type=jnp.float32)
    here = []
    for k in range(2):
        place = jnp.sum(before * hits[k], axis=0, keepdims=True)
        own_key = route[k : k + 1, :].astype(jnp.float32) * PAIR_KEY + (m * CAP + place)
        here.append((keys == own_key).astype(jnp.float32))
    return hits, named, here


def tables_kernel(dims, where_ref, routes_ref, probs_ref, tokens_ref, *refs):
    dp, cap2, experts = dims
    sent, aux_ref = refs[:dp], refs[dp]
    device = block_device(dims, routes_ref.shape[2], where_ref[0])
    micro = routes_ref.shape[0]
    blocks = tokens_ref.shape[2] // LANES
    aux_ref[...] = jnp.zeros_like(aux_ref)
    slots = jnp.zeros((dp * cap2, tokens_ref.shape[2]), jnp.float32)
    for m in range(micro):
        _, named, here = places(dims, device, routes_ref, m)
        pick = (here[0] + here[1]).astype(jnp.bfloat16)
        slots = slots + jnp.dot(pick, tokens_ref[m], preferred_element_type=jnp.float32)
        sums = jnp.sum(probs_ref[m], axis=1, keepdims=True)
        aux_ref[0:experts, m : m + 1] = jnp.sum(named, axis=1, keepdims=True)
        for piece in range(3):
            part = sums.astype(jnp.bfloat16).astype(jnp.float32)
            column = (piece + 1) * micro + m
            aux_ref[0:experts, column : column + 1] = part
            sums = sums - part
    slots = slots.astype(jnp.bfloat16)
    aux = aux_ref[...].astype(jnp.bfloat16)
    for d in range(dp):
        for b in range(blocks):
            sent[d][b * cap2 : (b + 1) * cap2, :] = slots[
                d * cap2 : (d + 1) * cap2, b * LANES : (b + 1) * LANES
            ]
        sent[d][blocks * cap2 :, :] = aux


def weights_kernel(dims, where_ref, routes_ref, probs_ref, after_ref, *orders):
    dp, cap2, experts = dims
    micro, _, rows = routes_ref.shape
    for shifted, pieces_ref in enumerate(orders):
        device = block_device(dims, rows, where_ref[0] if shifted else None)
        for m in range(micro):
            hits, _, here = places(dims, device, routes_ref, m)
            picked = [jnp.sum(probs_ref[m] * hit, axis=0, keepdims=True) for hit in hits]
            total = picked[0] + picked[1]
            left = (here[0] * (picked[0] / total) + here[1] * (picked[1] / total)).T
            for piece in range(3):
                part = left.astype(jnp.bfloat16)
                at = (piece * micro + m) * rows
                pieces_ref[at : at + rows, :] = part
                left = left - part.astype(jnp.float32)


def repack_kernel(dims, where_ref, *refs):
    dp, blocks, tokens_all, count = dims
    arrived, refs = refs[:dp], refs[dp:]
    xs, loss_ref, aux_ref = refs[:count], refs[count], refs[count + 1]
    experts, micro = loss_ref.shape
    cap2 = xs[0].shape[1]
    per = blocks // count
    for shift in range(dp):
        group = where_ref[0] ^ shift
        for b in range(blocks):
            xs[b // per][group, :, b % per * LANES : (b % per + 1) * LANES] = arrived[shift][
                b * cap2 : (b + 1) * cap2, :
            ]
        aux_ref[group] = arrived[shift][blocks * cap2 :, :].astype(jnp.float32)
    total = jnp.zeros((experts, LANES), jnp.float32)
    for group in range(dp):
        total = total + aux_ref[group]
    count = total[:, 0:micro]
    prob = total[:, 3 * micro : 4 * micro] + total[:, 2 * micro : 3 * micro]
    prob = prob + total[:, micro : 2 * micro]
    loss_ref[...] = experts * (count / (tokens_all * 2)) * (prob / tokens_all)


def gate_up_copies(pieces, here, sources, targets, sems):
    copies = []
    depth = targets[0].shape[0] // len(pieces)
    half = depth // 2
    for i, (quarter, c) in enumerate(pieces):
        start = ((here ^ quarter) * IN_CHUNKS + c) * depth
        for k, (source, target) in enumerate(zip(sources, targets)):
            for part in range(2):
                at = pl.multiple_of(start + part * half, half)
                copies.append(
                    pltpu.make_async_copy(
                        source.at[0, pl.ds(at, half), :],
                        target.at[pl.ds(i * depth + part * half, half), :],
                        sems.at[k, 2 * i + part],
                    )
                )
    return copies


def down_copies(side, parts, here, source, targets, sems):
    copies = []
    half, columns = targets[0].shape
    at = pl.multiple_of(((here >> 1) ^ side) * columns, columns)
    step = half // DOWN_PARTS
    for i, target in zip(parts, targets):
        for part in range(DOWN_PARTS):
            copies.append(
                pltpu.make_async_copy(
                    source.at[0, pl.ds(i * half + part * step, step), pl.ds(at, columns)],
                    target.at[pl.ds(part * step, step), :],
                    sems.at[i, part],
                )
            )
    return copies


def run_copies(copies):
    for copy in copies:
        copy.start()

    def finish():
        for copy in copies:
            copy.wait()

    return finish


def first_kernel(pieces, where_ref, after_ref, w_gate, w_up, gate_ref, up_ref, sems):
    sources, targets = (w_gate, w_up), (gate_ref, up_ref)
    run_copies(gate_up_copies(pieces, where_ref[0], sources, targets, sems))()


def gate_up_kernel(plan, where_ref, *refs):
    count, first, following, tile = plan
    last = following is None
    xs, refs = refs[:count], refs[count:]
    gate_w, up_w, refs = refs[0], refs[1], refs[2:]
    if not first:
        gate_in, up_in, refs = refs[0], refs[1], refs[2:]
    here = where_ref[0]
    if last:
        w_down, out_ref, next_a, next_b, sems = refs
        copies = down_copies(1, (0, 1), here, w_down, (next_a, next_b), sems)
    else:
        w_gate, w_up, gate_out, up_out, next_a, next_b, sems = refs
        copies = gate_up_copies(following, here, (w_gate, w_up), (next_a, next_b), sems)
    finish = run_copies(copies)
    depth = gate_w.shape[0] // count

    def step(j, carry):
        columns = pl.ds(pl.multiple_of(j * tile, tile), tile)
        if first:
            gate = up = 0.0
        else:
            gate, up = gate_in[:, columns], up_in[:, columns]
        for i, x in enumerate(xs):
            rows = slice(i * depth, (i + 1) * depth)
            gate = gate + jnp.dot(
                x[...], gate_w[rows, columns], preferred_element_type=jnp.float32
            )
            up = up + jnp.dot(x[...], up_w[rows, columns], preferred_element_type=jnp.float32)
        if last:
            out_ref[:, columns] = (gate / (1.0 + jnp.exp(-gate)) * up).astype(jnp.bfloat16)
        else:
            gate_out[:, columns] = gate
            up_out[:, columns] = up
        return carry

    lax.fori_loop(0, gate_w.shape[1] // tile, step, 0)
    finish()


VMEM = pl.BlockSpec(memory_space=pltpu.VMEM)
SMEM = pl.BlockSpec(memory_space=pltpu.SMEM)
HBM = pl.BlockSpec(memory_space=pltpu.HBM)


def first_weights(where, pieces, after, w_gate, w_up, depth):
    width = w_gate.shape[2]
    return pl.pallas_call(
        functools.partial(first_kernel, pieces),
        in_specs=[SMEM, pl.BlockSpec(memory_space=pl.ANY), HBM, HBM],
        out_specs=[VMEM] * 2,
        out_shape=[pltpu.VMEM((depth, width), jnp.bfloat16)] * 2,
        scratch_shapes=[pltpu.SemaphoreType.DMA((2, 2 * len(pieces)))],
        compiler_params=pltpu.CompilerParams(vmem_limit_bytes=1 << 20),
        name="first",
    )(where, after, w_gate, w_up)


def gate_up(where, xs, weights, totals, following, w_gate, w_up, w_down):
    rows = xs[0].shape[0]
    depth, width = weights[0].shape
    last = following is None
    if last:
        sources = [w_down]
        out_shape = [pltpu.VMEM((rows, width), jnp.bfloat16)]
        out_shape += [pltpu.VMEM((width // 2, w_down.shape[2] // 2), jnp.bfloat16)] * 2
    else:
        sources = [w_gate, w_up]
        out_shape = [pltpu.VMEM((rows, width), jnp.float32)] * 2
        out_shape += [pltpu.VMEM((depth, width), jnp.bfloat16)] * 2
    plan = (len(xs), totals is None, following, tile_of(width, (5 << 20) // (8 * rows)))
    totals = totals or []
    at = 1 + len(xs) + 2
    return pl.pallas_call(
        functools.partial(gate_up_kernel, plan),
        in_specs=[SMEM] + [VMEM] * (len(xs) + 2 + len(totals)) + [HBM] * len(sources),
        out_specs=[VMEM] * len(out_shape),
        out_shape=out_shape,
        scratch_shapes=[pltpu.SemaphoreType.DMA((2, max(4, DOWN_PARTS)))],
        input_output_aliases={} if last or not totals else {at + i: i for i in range(2)},
        compiler_params=pltpu.CompilerParams(vmem_limit_bytes=8 << 20),
        cost_estimate=pl.CostEstimate(
            flops=4 * rows * depth * width, transcendentals=0, bytes_accessed=4 * depth * width
        ),
    )(where, *xs, *weights, *totals, *sources)


def down_kernel(plan, where_ref, h_ref, w_a, w_b, after_ref, *refs):
    c, part, tile, columns = plan
    here = where_ref[0]
    if part is None:
        keep_ref, send_ref, token_ref = refs
        finish = None
    else:
        w_down, keep_ref, send_ref, token_ref, next_ref, sems = refs
        finish = run_copies(down_copies(0, (part,), here, w_down, (next_ref,), sems))
    quarter = columns * OUT_CHUNKS
    half = w_a.shape[0]

    def step(j, carry):
        for p, out_ref in enumerate((keep_ref, send_ref)):
            start = ((here & 1) ^ p) * quarter + c * columns
            at = pl.ds(pl.multiple_of(start + j * tile, tile), tile)
            total = jnp.dot(h_ref[:, :half], w_a[:, at], preferred_element_type=jnp.float32)
            total = total + jnp.dot(
                h_ref[:, half:], w_b[:, at], preferred_element_type=jnp.float32
            )
            out_ref[:, pl.ds(pl.multiple_of(j * tile, tile), tile)] = total.astype(out_ref.dtype)
        return carry

    lax.fori_loop(0, columns // tile, step, 0)
    token_ref[...] = jnp.zeros_like(token_ref)
    if finish is not None:
        finish()


def down(where, c, h, weights, after, part, w_down):
    rows, depth = h.shape
    half, both = weights[0].shape
    columns = both // 2 // OUT_CHUNKS
    out_shape = [
        pltpu.VMEM((rows, columns), jnp.float32),
        pltpu.VMEM((rows, columns), jnp.bfloat16),
        jax.ShapeDtypeStruct((8, LANES), jnp.float32),
    ]
    more = part is not None
    if more:
        out_shape.append(pltpu.VMEM((half, both), jnp.bfloat16))
    return pl.pallas_call(
        functools.partial(down_kernel, (c, part, tile_of(columns, 256), columns)),
        in_specs=[SMEM, VMEM, VMEM, VMEM, HBM] + [HBM] * more,
        out_specs=[VMEM] * len(out_shape),
        out_shape=out_shape,
        scratch_shapes=[pltpu.SemaphoreType.DMA((2, DOWN_PARTS))] * more,
        compiler_params=pltpu.CompilerParams(vmem_limit_bytes=8 << 20),
        cost_estimate=pl.CostEstimate(
            flops=4 * rows * depth * columns, transcendentals=0, bytes_accessed=4 * depth * columns
        ),
    )(where, h, *weights, after, *([w_down] * more))


def spread_kernel(dp, where_ref, keep_ref, got_ref, crossed_ref, *outs):
    for shift in range(dp):
        group = where_ref[0] ^ shift
        total = keep_ref[group] + got_ref[group].astype(jnp.float32)
        total = total + crossed_ref[group].astype(jnp.float32)
        outs[shift][...] = total.astype(jnp.bfloat16)


def combine_rows(pieces, part, out_ref, at):
    micro, rows, _ = out_ref.shape
    each = micro * rows
    width = part.shape[1]
    total = jnp.dot(pieces[...], part[...], preferred_element_type=jnp.float32)
    total = (total[2 * each :] + total[each : 2 * each]) + total[:each]
    total = total.astype(jnp.bfloat16)
    for m in range(micro):
        out_ref[m, :, at : at + width] = total[m * rows : (m + 1) * rows]


def half_kernel(pieces_ref, part_ref, out_ref):
    combine_rows(pieces_ref, part_ref, out_ref, 0)


def combine_kernel(half_ref, pieces_ref, *refs):
    blocks, out_ref, rows_ref = refs[:-2], refs[-2], refs[-1]
    cap2 = blocks[0].shape[0]
    width = half_ref.shape[2]
    out_ref[:, :, :width] = half_ref[...]
    for shift, block in enumerate(blocks):
        rows_ref[shift * cap2 : (shift + 1) * cap2, :] = block[...]
    combine_rows(pieces_ref, rows_ref, out_ref, width)


def local(dp, tensor, tokens, routes, probs, w_gate, w_up, w_down):
    micro, rows, features = tokens.shape
    experts = probs.shape[-1]
    cap2 = micro * CAP
    blocks = features // LANES
    slots_all = dp * cap2
    where = lax.axis_index("tensor")[None]
    w_gate, w_up, w_down = (
        pltpu.with_memory_space_constraint(w, pltpu.HBM) for w in (w_gate, w_up, w_down)
    )
    core = [(t, t ^ 1) for t in range(tensor)]
    row = [(t, t ^ 2) for t in range(tensor)]

    width = features // IN_CHUNKS
    dims = (dp, cap2, experts)
    routes, probs = routes.transpose(0, 2, 1), probs.transpose(0, 2, 1)
    place = lax.axis_index("dp")[None]
    inputs = (pltpu.with_memory_space_constraint(a, pltpu.HBM) for a in (routes, probs, tokens))
    sent = pl.pallas_call(
        functools.partial(tables_kernel, dims),
        in_specs=[SMEM] + [VMEM] * 3,
        out_shape=[pltpu.VMEM((blocks * cap2 + experts, LANES), jnp.bfloat16)] * dp,
        scratch_shapes=[pltpu.VMEM((experts, LANES), jnp.float32)],
        compiler_params=pltpu.CompilerParams(vmem_limit_bytes=48 << 20),
        name="tables",
    )(place, *inputs)
    arrived = [sent[0]] * dp
    for shift in reversed(range(1, dp)):
        swap = [(i, i ^ shift) for i in range(dp)]
        arrived[shift] = lax.ppermute(sent[shift], "dp", swap)
    chunks = range(IN_CHUNKS)
    stages = [[(q, c) for c in chunks] for q in range(2)] + [[(2, c), (3, c)] for c in chunks]
    weights = first_weights(where, stages[0], sent[0], w_gate, w_up, features)
    *xs, loss = pl.pallas_call(
        functools.partial(repack_kernel, (dp, blocks, rows * dp, IN_CHUNKS)),
        in_specs=[SMEM] + [VMEM] * dp,
        out_shape=[pltpu.VMEM((dp, cap2, width), jnp.bfloat16)] * IN_CHUNKS
        + [jax.ShapeDtypeStruct((experts, micro), jnp.float32)],
        scratch_shapes=[pltpu.VMEM((dp, experts, LANES), jnp.float32)],
        compiler_params=pltpu.CompilerParams(vmem_limit_bytes=12 << 20),
        name="repack",
    )(place, *arrived)
    xs = [x.reshape(slots_all, width) for x in xs]
    paired, crossed = [], []
    for x in xs:
        paired.append(lax.ppermute(x, "tensor", core))
        crossed.append(lax.ppermute(x, "tensor", row))
    operands = [xs, paired]
    for c in chunks:
        operands.append([crossed[c], lax.ppermute(crossed[c], "tensor", core)])
    totals = None
    for at, pieces in enumerate(operands):
        following = stages[at + 1] if at + 1 < len(stages) else None
        made = gate_up(where, pieces, weights, totals, following, w_gate, w_up, w_down)
        totals, weights = made[:-2], made[-2:]
    hidden = totals[0]

    returned = []
    kept = {}
    width = features // OUT_CHUNKS
    token = loss
    for side in (1, 0):
        upcoming = []
        for c in range(OUT_CHUNKS):
            keep, send, token, *more = down(
                where, c, hidden, weights, token, c if side else None, w_down
            )
            upcoming += more
            kept[side, c] = (keep, lax.ppermute(send, "tensor", core))
        weights = upcoming
    combine = pl.pallas_call(
        functools.partial(weights_kernel, dims),
        in_specs=[SMEM] + [VMEM] * 2 + [pl.BlockSpec(memory_space=pl.ANY)],
        out_shape=[jax.ShapeDtypeStruct((3 * micro * rows, slots_all), jnp.bfloat16)] * 2,
        compiler_params=pltpu.CompilerParams(vmem_limit_bytes=8 << 20),
        name="weights",
    )(place, routes, probs, token)
    crossed = []
    for c in range(OUT_CHUNKS):
        keep, got = kept[1, c]
        total = (keep + got.astype(jnp.float32)).astype(jnp.bfloat16)
        crossed.append(lax.ppermute(total, "tensor", row))
    keep, got = kept[0, 0]
    total = keep + got.astype(jnp.float32) + crossed[0].astype(jnp.float32)
    total = total.astype(jnp.bfloat16).reshape(dp, cap2, width)
    back = lax.all_to_all(total, "dp", split_axis=0, concat_axis=0, tiled=True)
    returned.append(
        pltpu.with_memory_space_constraint(back.reshape(slots_all, width), pltpu.VMEM)
    )
    blocks = pl.pallas_call(
        functools.partial(spread_kernel, dp),
        in_specs=[SMEM] + [VMEM] * 3,
        out_shape=[jax.ShapeDtypeStruct((cap2, width), jnp.bfloat16)] * dp,
        compiler_params=pltpu.CompilerParams(vmem_limit_bytes=12 << 20),
        name="spread",
    )(place, *(a.reshape(dp, cap2, width) for a in (*kept[0, 1], crossed[1])))
    home = [blocks[0]] * dp
    for shift in reversed(range(1, dp)):
        swap = [(i, i ^ shift) for i in range(dp)]
        home[shift] = lax.ppermute(blocks[shift], "dp", swap)
    half = pl.pallas_call(
        half_kernel,
        out_shape=jax.ShapeDtypeStruct((micro, rows, width), jnp.bfloat16),
        compiler_params=pltpu.CompilerParams(vmem_limit_bytes=16 << 20),
        name="half",
    )(combine[0], *returned)
    mixed = pl.pallas_call(
        combine_kernel,
        out_shape=jax.ShapeDtypeStruct((micro, rows, features), jnp.bfloat16),
        scratch_shapes=[pltpu.VMEM((slots_all, width), jnp.bfloat16)],
        compiler_params=pltpu.CompilerParams(vmem_limit_bytes=16 << 20),
        name="combine",
    )(half, combine[1], *home)
    return mixed, loss.T


def solution(mesh):
    dp, tensor = mesh.shape["dp"], mesh.shape["tensor"]
    in_specs = (
        P(None, "dp", "tensor"),
        P(None, "dp", None),
        P(None, "dp", None),
        P("dp", None, "tensor"),
        P("dp", None, "tensor"),
        P("dp", "tensor", None),
    )
    out_specs = (P(None, "dp", "tensor"), P())


    def body(*args):
        return local(dp, tensor, *args)

    return jax.shard_map(
        body, mesh=mesh, in_specs=in_specs, out_specs=out_specs, check_vma=False
    )
```
